32 devices in a mesh: prompt: 4 (over y, core), seq: 4 (over z), head: 2 (over x).
Axes of the slice: x: 2, y: 2, z: 4, core: 2. Of those that a mesh axis runs over, the one named last changes fastest.
Arguments:
- queries: bfloat16 [16, 64, 1280], P(('prompt', 'seq'), None, 'head'), parts along dimension 0, may hold values from -1024 to 1024
- prefix_keys: bfloat16 [65536, 256], P(('prompt', 'seq'), 'head'), parts along dimension 0, may hold values from -6 to 6
- prefix_values: bfloat16 [65536, 256], P(('prompt', 'seq'), 'head'), parts along dimension 0, may hold values from -6 to 6
- suffix_keys: bfloat16 [16, 2048, 256], P(('prompt', 'seq'), None, 'head'), parts along dimension 0, may hold values from -6 to 6
- suffix_values: bfloat16 [16, 2048, 256], P(('prompt', 'seq'), None, 'head'), parts along dimension 0, may hold values from -6 to 6
- kept_blocks: int32 [16, 16], P('prompt'), parts along dimension 0, may hold values from 0 to 127, as said below
- suffix_lengths: int32 [16], P(('prompt', 'seq')), parts along dimension 0, may hold values from 64 to 2048, as said below
- out_weight: bfloat16 [1280, 5120], P('head', 'seq'), may hold values from -1.75 to 1.75
Outputs:
- projected: float32 [1024, 5120], P(('prompt', 'head'), 'seq'), parts along dimension 0
The draws below stay inside these ranges and needn't reach their ends.
There are 4 independent parts, one for each index of `prompt`. The reference program is written for one: setup_inputs(seed, part) draws one part's arguments, and reference() takes and returns one part's arrays. A program takes and returns all parts, laid end to end along the dimension named above; an argument that names none is the same for every part. Nothing has to cross between parts.
Inputs may be any that keep to these rules, and one draw needn't show every extreme that they name: `kept_blocks`: each row names 16 different prefix blocks. Among the blocks k * 32 to (k + 1) * 32 - 1, for each k, at most 8 are named by one row, and every row names exactly 8 of one such run. `suffix_lengths`: A sample's query tokens are the last 64 of its filled slots; some sample fills all 2048.
All inputs are finite; a program needn't handle non-finite values.
Results may differ from the reference program's by a relative error of at most 0.008.
Values may be sent and summed in bfloat16 or wider, within the bound.
A program may use at most 64 MiB of HBM per device.

```python
import math
import jax
import jax.numpy as jnp
from jax import lax

D = 5120
HD = 128
GQA = 5
QB = 64
BLOCK = 128
MOST = 8
SUF = 2048
BLK_DEV = 32
KVH = 2
QH = 10
SAMPLES = 4
TOKENS = 256
NBLK = 128
NTOK = 16384
KEEP = 16
N_SEQ = 4


def key_field(key):
    return jnp.clip(jax.random.normal(jax.random.fold_in(key, 3), (NTOK, KVH * HD), jnp.float32), -6.0, 6.0)


def kept_field(key):
    root = jax.random.fold_in(key, 7)

    def one_sample(sample_key):
        part_a, part_b, part_c, part_d = jax.random.split(sample_key, 4)
        placing = jax.random.permutation(part_a, N_SEQ)
        paired = jax.random.randint(part_b, (N_SEQ // 2,), 0, MOST + 1)
        paired = paired.at[0].set(MOST)
        by_rank = jnp.stack([paired, MOST - paired], axis=1).reshape(N_SEQ)
        counts = jnp.zeros((N_SEQ,), jnp.int32).at[placing].set(by_rank)
        local_order = jax.vmap(lambda inner: jax.random.permutation(inner, BLK_DEV))(jax.random.split(part_c, N_SEQ))
        numbers = jnp.arange(N_SEQ, dtype=jnp.int32)[:, None] * BLK_DEV + local_order.astype(jnp.int32)
        living = jnp.arange(BLK_DEV, dtype=jnp.int32)[None, :] < counts[:, None]
        ranked = jnp.argsort(jnp.where(living, 0, 1).astype(jnp.int32).reshape(-1), stable=True)[:KEEP]
        picked = numbers.reshape(-1)[ranked]
        return jax.random.permutation(part_d, picked)
    return jax.vmap(one_sample)(jax.random.split(root, SAMPLES)).astype(jnp.int32)


def draw_prefix_keys(key, part):
    return key_field(key).astype(jnp.bfloat16)


def draw_kept_blocks(key, part):
    return kept_field(key)


def draw_suffix_lengths(key, part):
    first_key, second_key = jax.random.split(jax.random.fold_in(key, 5))
    lengths = jax.random.randint(first_key, (SAMPLES,), QB, SUF + 1)
    spot = jax.random.randint(second_key, (), 0, SAMPLES)
    return lengths.at[spot].set(SUF).astype(jnp.int32)


def draw_queries(key, part):
    result = 1.5 * jnp.clip(jax.random.normal(jax.random.fold_in(key, 11), (SAMPLES, QB, QH * HD), jnp.float32), -6.0, 6.0)
    return result.astype(jnp.bfloat16)


def steps_of(rng, shape, shards, low, largest):
    loudness, own = 1.0, jax.random.fold_in(rng, 6)
    for position, blocks in shards:
        draws = jnp.exp(jax.random.uniform(jax.random.fold_in(own, position), (blocks,), jnp.float32, low / len(shards), largest / len(shards)))
        loudness = loudness * jnp.repeat(draws, shape[position] // blocks).reshape([-1 if axis == position else 1 for axis in range(len(shape))])
    return loudness


def centred(rng, extent, width, bound, shards=(), kind=jnp.bfloat16):
    drawn = width * jax.random.normal(rng, extent, jnp.float32)
    if shards:
        drawn = drawn * steps_of(rng, extent, shards, -0.22, 0.18)
    return jnp.clip(drawn, -bound, bound).astype(kind)


def setup_inputs(seed: int = 0, part: int = 0) -> dict:
    keys = jax.random.split(jax.random.key(seed), 9)
    part_splits = jax.random.split(jax.random.fold_in(keys[8], part), 9)
    return {
        "queries": draw_queries(jax.random.fold_in(jax.random.fold_in(keys[8], part), 71), part),
        "prefix_keys": draw_prefix_keys(jax.random.fold_in(jax.random.fold_in(keys[8], part), 71), part),
        "prefix_values": centred(part_splits[2], (NTOK, KVH * HD), 1.0, 6.0, ((0, 4), (1, 2))),
        "suffix_keys": centred(part_splits[3], (SAMPLES, SUF, KVH * HD), 1.0, 6.0, ((0, 4), (2, 2))),
        "suffix_values": centred(part_splits[4], (SAMPLES, SUF, KVH * HD), 1.0, 6.0, ((0, 4), (2, 2))),
        "kept_blocks": draw_kept_blocks(jax.random.fold_in(jax.random.fold_in(keys[8], part), 71), part),
        "suffix_lengths": draw_suffix_lengths(jax.random.fold_in(jax.random.fold_in(keys[8], part), 71), part),
        "out_weight": centred(keys[7], (QH * HD, D), (8.0 / D ** 0.5), 1.75, ((0, 2), (1, 4))),
    }


def reference(queries, prefix_keys, prefix_values, suffix_keys, suffix_values, kept_blocks, suffix_lengths, out_weight):
    kv_heads = prefix_keys.shape[1] // HD
    scaling = 1.0 / math.sqrt(HD)
    block_keys = prefix_keys.reshape(NBLK, BLOCK, kv_heads, HD)
    block_values = prefix_values.reshape(NBLK, BLOCK, kv_heads, HD)

    def attend_sample(sample_id):
        kept_ids = kept_blocks[sample_id]
        key_rows = jnp.concatenate([block_keys[kept_ids].reshape(KEEP * BLOCK, kv_heads, HD), suffix_keys[sample_id].reshape(SUF, kv_heads, HD)], 0)
        value_rows = jnp.concatenate([block_values[kept_ids].reshape(KEEP * BLOCK, kv_heads, HD), suffix_values[sample_id].reshape(SUF, kv_heads, HD)], 0)
        asking = queries[sample_id].reshape(QB, kv_heads, GQA, HD)
        scores = jnp.einsum('tgjd,sgd->tgjs', asking.astype(jnp.float32), key_rows.astype(jnp.float32)) * scaling
        slot_pos = jnp.arange(SUF, dtype=jnp.int32)
        last_seen = suffix_lengths[sample_id] - QB + jnp.arange(QB, dtype=jnp.int32)
        own_mask = slot_pos[None, :] <= last_seen[:, None]
        visible = jnp.concatenate([jnp.ones((QB, KEEP * BLOCK), dtype=bool), own_mask], 1)[:, None, None, :]
        maximum = lax.optimization_barrier(jnp.max(jnp.where(visible, scores, -jnp.inf), axis=-1, keepdims=True))
        weights = jnp.where(visible, jnp.exp(scores - maximum), 0.0).astype(jnp.bfloat16)
        weight_sum = lax.optimization_barrier(jnp.sum(weights.astype(jnp.float32), axis=-1))
        summed = jnp.einsum('tgjs,sgd->tgjd', weights.astype(jnp.float32), value_rows.astype(jnp.float32))
        return (summed / weight_sum[..., None]).astype(jnp.bfloat16).reshape(QB, kv_heads * GQA * HD)
    attended = lax.map(attend_sample, jnp.arange(SAMPLES, dtype=jnp.int32)).reshape(TOKENS, -1)
    return jnp.dot(attended, out_weight, preferred_element_type=jnp.float32)
```

```python
import functools
import math

import jax
import jax.numpy as jnp
from jax import lax
from jax.experimental import pallas as pl
from jax.experimental.pallas import tpu as pltpu
from jax.sharding import PartitionSpec as P

HD = 128
GQA = 5
BLOCK = 128
MOST = 8
CHUNK = MOST * BLOCK

floor_value = -1e30
hidden_value = -3e30
factor = math.log2(math.e) / math.sqrt(HD)


def chosen_slots(kept, sample, base, blocks_here):
    slots = [jnp.int32(0)] * MOST
    count = jnp.int32(0)
    for e in range(kept.shape[1]):
        local = kept[sample, e] - base
        present = (local >= 0) & (local < blocks_here)
        rank = jnp.where(present, count, -1)
        slots = [jnp.where(rank == j, local, slots[j]) for j in range(MOST)]
        count = count + jnp.where(present, 1, 0)
    return slots, count


def rows_of(block):
    return jnp.concatenate([block[:, j * HD : (j + 1) * HD] for j in range(GQA)], axis=0)


def scores_of(asking, keys):
    return lax.dot_general(asking, keys, (((1,), (1,)), ((), ())), preferred_element_type=jnp.float32)


def softmax_part(scores, values):
    maximum = jnp.maximum(jnp.max(scores, axis=-1, keepdims=True), floor_value)
    weights = jnp.exp2((scores - maximum) * factor).astype(jnp.bfloat16)
    weight_sum = jnp.sum(weights.astype(jnp.float32), axis=-1, keepdims=True)
    return maximum, weight_sum, jnp.dot(weights, values, preferred_element_type=jnp.float32)


def kernel(
    n, heads,
    q_hbm, pk_hbm, pv_hbm, sk_hbm, sv_hbm, kept, lengths, w_hbm,
    out,
    qbuf, pk, pv, sk, sv, wall, own_acc, own_max, own_sum, psend, pbuf, ssend, sbuf, att, fbuf,
    lsem, q_s, q_r, p_s, p_r, s_s, s_r, a_s, a_r, f_s, f_r, w_s, w_r, v_s, v_r,
):
    me = lax.axis_index("seq")
    head = lax.axis_index("head")
    prompt = lax.axis_index("prompt")
    side = prompt % 2
    twin = prompt + 1 - 2 * side
    tokens = q_hbm.shape[0]
    blocks_here = pk_hbm.shape[0]
    base = me * blocks_here
    per_head = n // heads

    def partner(r):
        found, bit = 0, 1
        while bit < n:
            found = found + (me // bit + r // bit) % 2 * bit
            bit *= 2
        return found

    def turn(i):
        return (i + n // 2 - 1) % (n - 1) + 1

    loads = [
        pltpu.make_async_copy(src, dst, lsem.at[i])
        for i, (src, dst) in enumerate(
            ((q_hbm, qbuf.at[0]), (sk_hbm, sk), (sv_hbm, sv), (pk_hbm, pk), (pv_hbm, pv), (w_hbm, wall.at[head]))
        )
    ]
    for load in loads:
        load.start()

    barrier = pltpu.get_barrier_semaphore()
    for r in range(1, n):
        pl.semaphore_signal(barrier, inc=1, device_id={"seq": partner(r)})
    for r in range(1, heads):
        pl.semaphore_signal(barrier, inc=1, device_id={"head": lax.rem(head + r, heads)})
    pl.semaphore_signal(barrier, inc=1, device_id={"prompt": twin})
    pl.semaphore_wait(barrier, n - 1 + heads - 1 + 1)

    def query_copy(r):
        return pltpu.make_async_remote_copy(
            qbuf.at[0], qbuf.at[r], q_s.at[r], q_r.at[r], device_id={"seq": partner(r)}
        )

    def part_copy(r):
        return pltpu.make_async_remote_copy(
            psend.at[r], pbuf.at[r], p_s.at[r], p_r.at[r], device_id={"seq": partner(r)}
        )

    def stat_copy(r):
        return pltpu.make_async_remote_copy(
            ssend.at[r], sbuf.at[r], s_s.at[r], s_r.at[r], device_id={"seq": partner(r)}
        )

    def attended_copy(r, sample):
        return pltpu.make_async_remote_copy(
            att.at[sample], att.at[sample], a_s.at[r], a_r.at[sample], device_id={"seq": partner(r)}
        )

    def forward_copy(r, sample):
        place = lax.rem(sample, per_head)
        return pltpu.make_async_remote_copy(
            att.at[sample], fbuf.at[r, place], f_s.at[r, place], f_r.at[r, place],
            device_id={"head": lax.rem(head + r, heads)},
        )

    half = w_hbm.shape[0] // 2

    def source(r):
        return lax.rem(head + heads - r, heads)

    def weight_copy(r, owner):
        place = wall.at[owner, pl.ds(side * half, half)]
        return pltpu.make_async_remote_copy(
            place, place, w_s.at[r], w_r.at[r], device_id={"head": lax.rem(head + r, heads)}
        )

    def twin_copy(r, which):
        place = wall.at[source(r), pl.ds(which * half, half)]
        return pltpu.make_async_remote_copy(place, place, v_s.at[r], v_r.at[r], device_id={"prompt": twin})

    loads[0].wait()
    for i in range(n - 1):
        query_copy(turn(i)).start()
    loads[5].wait()
    for r in range(1, heads):
        weight_copy(r, head).start()

    def prefix_part(asking, sample):
        slots, count = chosen_slots(kept, sample, base, blocks_here)
        keys = jnp.concatenate([pk[slot] for slot in slots], axis=0)
        values = jnp.concatenate([pv[slot] for slot in slots], axis=0)
        column = lax.broadcasted_iota(jnp.int32, (1, CHUNK), 1)
        hidden = jnp.where(column < count * BLOCK, 0.0, hidden_value)
        return softmax_part(scores_of(asking, keys) + hidden, values)

    asking = rows_of(qbuf[0])
    rows = asking.shape[0]
    last_seen = lengths[0] - tokens + lax.broadcasted_iota(jnp.int32, (rows, 1), 0) % tokens
    loads[1].wait()
    loads[2].wait()

    def own_scores(keys, start):
        column = start + lax.broadcasted_iota(jnp.int32, (1, keys.shape[0]), 1)
        return jnp.where(column <= last_seen, scores_of(asking, keys), hidden_value)

    def merged(one, two):
        maximum = jnp.maximum(one[0], two[0])
        shrink_one = jnp.exp2((one[0] - maximum) * factor)
        shrink_two = jnp.exp2((two[0] - maximum) * factor)
        return (
            maximum,
            one[1] * shrink_one + two[1] * shrink_two,
            one[2] * shrink_one + two[2] * shrink_two,
        )

    state = None
    for start in range(0, sk.shape[0], CHUNK):
        piece = pl.ds(start, min(CHUNK, sk.shape[0] - start))
        latest = softmax_part(own_scores(sk[piece], start), sv[piece])
        state = latest if state is None else merged(state, latest)
    loads[3].wait()
    loads[4].wait()
    state = merged(state, prefix_part(asking, me))
    own_max[...] = jnp.broadcast_to(state[0], own_max.shape)
    own_sum[...] = jnp.broadcast_to(state[1], own_sum.shape)
    own_acc[...] = state[2]

    lane = lax.broadcasted_iota(jnp.int32, (tokens, HD), 1)

    def remote_part(i, carry):
        r = turn(i)
        query_copy(r).wait_recv()
        maximum, weight_sum, summed = prefix_part(rows_of(qbuf[r]), partner(r))
        mean = (summed / jnp.maximum(weight_sum, 1e-30)).astype(jnp.bfloat16)
        stats = jnp.zeros((tokens, HD), jnp.float32)
        for j in range(GQA):
            piece = slice(j * tokens, (j + 1) * tokens)
            psend[r, :, j * HD : (j + 1) * HD] = mean[piece]
            stats = jnp.where(lane == j, maximum[piece], stats)
            stats = jnp.where(lane == GQA + j, weight_sum[piece], stats)
        part_copy(r).start()
        square = jnp.concatenate([stats, jnp.zeros((HD - tokens, HD), jnp.float32)], axis=0)
        ssend[r] = square.T[: ssend.shape[1]]
        stat_copy(r).start()
        return carry

    lax.fori_loop(0, n - 1, remote_part, 0)

    def stats_from(r):
        part_copy(r).wait_recv()
        stat_copy(r).wait_recv()
        padded = jnp.concatenate([sbuf[r], jnp.zeros((HD - sbuf.shape[1], HD), jnp.float32)], axis=0)
        return padded.T[:tokens]

    stats = [stats_from(r) for r in range(1, n)]
    for j in range(GQA):
        piece = pl.ds(j * tokens, tokens)
        columns = slice(j * HD, (j + 1) * HD)
        maximum = own_max[piece]
        for one in stats:
            maximum = jnp.maximum(maximum, one[:, j : j + 1])
        scale = jnp.exp2((own_max[piece] - maximum) * factor)
        total = own_acc[piece] * scale
        weight_sum = own_sum[piece] * scale
        for r, one in zip(range(1, n), stats):
            share = jnp.exp2((one[:, j : j + 1] - maximum) * factor) * one[:, GQA + j : GQA + j + 1]
            total = total + share * pbuf[r, :, columns].astype(jnp.float32)
            weight_sum = weight_sum + share
        att[me, :, columns] = (total / weight_sum).astype(jnp.bfloat16)
    for i in range(n - 1):
        attended_copy(turn(i), me).start()

    def forward(sample):
        reader = sample // per_head

        @pl.when(reader != head)
        def _():
            forward_copy(lax.rem(reader + heads - head, heads), sample).start()

    forward(me)
    for r in range(1, heads):
        weight_copy(r, source(r)).wait_recv()
        twin_copy(r, side).start()
    for i in range(n - 1):
        sample = partner(turn(i))
        attended_copy(turn(i), sample).wait_recv()
        forward(sample)

    def projected(block, owner):
        return jnp.dot(
            block.reshape(per_head * tokens, block.shape[-1]), wall[owner], preferred_element_type=jnp.float32
        )

    out[...] = projected(att[pl.ds(head * per_head, per_head)], head)
    for r in range(1, heads):
        twin_copy(r, 1 - side).wait_recv()
        for i in range(per_head):
            forward_copy(r, i).wait_recv()
        out[...] += projected(fbuf[r], source(r))

    for r in range(1, n):
        query_copy(r).wait_send()
        part_copy(r).wait_send()
        stat_copy(r).wait_send()
        attended_copy(r, me).wait_send()
    for r in range(1, heads):
        weight_copy(r, head).wait_send()
        twin_copy(r, side).wait_send()
        for i in range(per_head):
            forward_copy(r, i).wait_send()


def body(n, heads, queries, prefix_keys, prefix_values, suffix_keys, suffix_values, kept_blocks, suffix_lengths, out_weight):
    tokens, width = queries.shape[1:]
    blocks_here = prefix_keys.shape[0] // BLOCK
    slots = suffix_keys.shape[1]
    columns = out_weight.shape[1]
    per_head = n // heads
    assert prefix_keys.shape[1] == HD and width == GQA * HD and n % heads == 0
    assert n & (n - 1) == 0
    bf16, f32 = jnp.bfloat16, jnp.float32
    any_space = pl.BlockSpec(memory_space=pltpu.HBM)
    smem = pl.BlockSpec(memory_space=pltpu.SMEM)
    dma = pltpu.SemaphoreType.DMA
    return pl.pallas_call(
        functools.partial(kernel, n, heads),
        out_shape=pltpu.VMEM((per_head * tokens, columns), f32),
        in_specs=[any_space] * 5 + [smem] * 2 + [any_space],
        out_specs=pl.BlockSpec(memory_space=pltpu.VMEM),
        scratch_shapes=[
            pltpu.VMEM((n, tokens, width), bf16),
            pltpu.VMEM((blocks_here, BLOCK, HD), bf16),
            pltpu.VMEM((blocks_here, BLOCK, HD), bf16),
            pltpu.VMEM((slots, HD), bf16),
            pltpu.VMEM((slots, HD), bf16),
            pltpu.VMEM((heads,) + out_weight.shape, bf16),
            pltpu.VMEM((GQA * tokens, HD), f32),
            pltpu.VMEM((GQA * tokens, HD), f32),
            pltpu.VMEM((GQA * tokens, HD), f32),
            pltpu.VMEM((n, tokens, width), bf16),
            pltpu.VMEM((n, tokens, width), bf16),
            pltpu.VMEM((n, 16, HD), f32),
            pltpu.VMEM((n, 16, HD), f32),
            pltpu.VMEM((n, tokens, width), bf16),
            pltpu.VMEM((heads, per_head, tokens, width), bf16),
            dma((6,)),
            dma((n,)), dma((n,)),
            dma((n,)), dma((n,)),
            dma((n,)), dma((n,)),
            dma((n,)), dma((n,)),
            dma((heads, per_head)), dma((heads, per_head)),
            dma((heads,)), dma((heads,)),
            dma((heads,)), dma((heads,)),
        ],
        compiler_params=pltpu.CompilerParams(
            collective_id=0, has_side_effects=True, vmem_limit_bytes=63 * 1024 * 1024
        ),
    )(
        queries[0],
        prefix_keys.reshape(blocks_here, BLOCK, HD),
        prefix_values.reshape(blocks_here, BLOCK, HD),
        suffix_keys[0],
        suffix_values[0],
        kept_blocks,
        suffix_lengths,
        out_weight,
    )


def solution(mesh):
    in_specs = (
        P(("prompt", "seq"), None, "head"),
        P(("prompt", "seq"), "head"),
        P(("prompt", "seq"), "head"),
        P(("prompt", "seq"), None, "head"),
        P(("prompt", "seq"), None, "head"),
        P("prompt", None),
        P(("prompt", "seq")),
        P("head", "seq"),
    )
    out_specs = P(("prompt", "head"), "seq")
    part = functools.partial(body, mesh.shape["seq"], mesh.shape["head"])
    return jax.shard_map(part, mesh=mesh, in_specs=in_specs, out_specs=out_specs, check_vma=False)
```

```python
import functools
import math

import jax
import jax.numpy as jnp
from jax import lax
from jax.experimental import pallas as pl
from jax.experimental.pallas import tpu as pltpu
from jax.sharding import PartitionSpec as P

HD = 128
GQA = 5
BLOCK = 128
MOST = 8
CHUNK = MOST * BLOCK
SPLIT = 2

floor_value = -1e30
hidden_value = -3e30
factor = math.log2(math.e) / math.sqrt(HD)


def chosen_slots(kept, sample, base, blocks_here):
    slots = [jnp.int32(0)] * MOST
    count = jnp.int32(0)
    for e in range(kept.shape[1]):
        local = kept[sample, e] - base
        present = (local >= 0) & (local < blocks_here)
        rank = jnp.where(present, count, -1)
        slots = [jnp.where(rank == j, local, slots[j]) for j in range(MOST)]
        count = count + jnp.where(present, 1, 0)
    return slots, count


def rows_of(block):
    return jnp.concatenate([block[:, j * HD : (j + 1) * HD] for j in range(GQA)], axis=0)


def scores_of(asking, keys):
    return lax.dot_general(asking, keys, (((1,), (1,)), ((), ())), preferred_element_type=jnp.float32)


def softmax_part(scores, values):
    maximum = jnp.maximum(jnp.max(scores, axis=-1, keepdims=True), floor_value)
    weights = jnp.exp2((scores - maximum) * factor).astype(jnp.bfloat16)
    weight_sum = jnp.sum(weights.astype(jnp.float32), axis=-1, keepdims=True)
    return maximum, weight_sum, jnp.dot(weights, values, preferred_element_type=jnp.float32)


def low_bit(r):
    return r & -r


def lower_bits(r):
    return [bit for bit in (1 << k for k in reversed(range(16))) if bit < r]


def relay_order(n):
    return sorted((r for r in range(1, n) if low_bit(r) > 1), key=lambda r: (-low_bit(r), r))


def kernel(
    n, heads, prompts,
    q_hbm, pk_hbm, pv_hbm, sk_hbm, sv_hbm, kept, lengths, w_hbm,
    out,
    qbuf, pk, pv, sk, sv, wall, own_acc, own_max, own_sum, psend, pbuf, ssend, sbuf, att, fbuf, chosen,
    lsem, q_s, q_r, p_s, p_r, s_s, s_r, a_s, a_r, f_s, f_r, w_s, w_r, v_s, v_r,
):
    me = lax.axis_index("seq")
    head = lax.axis_index("head")
    prompt = lax.axis_index("prompt")
    tokens = q_hbm.shape[0]
    blocks_here = pk_hbm.shape[0]
    base = me * blocks_here
    per_head = n // heads
    piece = tokens // SPLIT

    def flipped(index, size, r):
        found, bit = 0, 1
        while bit < size:
            found = found + (index // bit + r // bit) % 2 * bit
            bit *= 2
        return found

    def partner(r):
        return flipped(me, n, r)

    def span(h):
        return pl.ds(h * piece, piece)

    loads = [
        pltpu.make_async_copy(src, dst, lsem.at[i])
        for i, (src, dst) in enumerate(
            ((q_hbm, qbuf.at[0]), (sk_hbm, sk), (sv_hbm, sv), (pk_hbm, pk), (pv_hbm, pv), (w_hbm, wall.at[head]))
        )
    ]
    for load in loads:
        load.start()

    barrier = pltpu.get_barrier_semaphore()
    for r in range(1, n):
        pl.semaphore_signal(barrier, inc=1, device_id={"seq": partner(r)})
    for r in range(1, heads):
        other = lax.rem(head + r, heads)
        pl.semaphore_signal(barrier, inc=1, device_id={"head": other})
        pl.semaphore_signal(barrier, inc=1, device_id={"head": other, "seq": partner(1)})
    for bit in lower_bits(prompts):
        pl.semaphore_signal(barrier, inc=1, device_id={"prompt": flipped(prompt, prompts, bit)})

    def choose(sample, carry):
        slots, count = chosen_slots(kept, sample, base, blocks_here)
        for j in range(MOST):
            chosen[sample, j] = slots[j]
        chosen[sample, MOST] = count
        return carry

    lax.fori_loop(0, n, choose, 0)
    pl.semaphore_wait(barrier, n - 1 + 2 * (heads - 1) + len(lower_bits(prompts)))

    def query_copy(r, h, low):
        return pltpu.make_async_remote_copy(
            qbuf.at[r - low, span(h)], qbuf.at[r, span(h)], q_s.at[r, h], q_r.at[r, h], device_id={"seq": partner(low)}
        )

    def part_copy(r, h):
        return pltpu.make_async_remote_copy(
            psend.at[r, span(h)], pbuf.at[r, span(h)], p_s.at[r, h], p_r.at[r, h], device_id={"seq": partner(r)}
        )

    def stat_copy(r, h):
        return pltpu.make_async_remote_copy(
            ssend.at[r, h], sbuf.at[r, h], s_s.at[r, h], s_r.at[r, h], device_id={"seq": partner(r)}
        )

    def attended_copy(r, h):
        low = low_bit(r)
        return pltpu.make_async_remote_copy(
            att.at[r - low, span(h)], att.at[r, span(h)], a_s.at[r, h], a_r.at[r, h], device_id={"seq": partner(low)}
        )

    def place_of(r):
        sample = partner(r)
        return sample // per_head, lax.rem(sample, per_head)

    def final_copy(r, h, across):
        reader, place = place_of(r)
        return pltpu.make_async_remote_copy(
            att.at[r, span(h)], fbuf.at[head, place, span(h)], f_s.at[r // 2, across, h], f_r.at[head, place, h],
            device_id={"head": reader, "seq": partner(1) if across else me},
        )

    def arrival(g, place, h):
        spot = fbuf.at[g, place, span(h)]
        return pltpu.make_async_remote_copy(
            spot, spot, f_s.at[0, 0, h], f_r.at[g, place, h], device_id={"seq": partner(1)}
        )

    def source(r):
        return lax.rem(head + heads - r, heads)

    share = w_hbm.shape[0] // (prompts * SPLIT)

    def weight_place(owner, k, c):
        return wall.at[owner, pl.ds((flipped(prompt, prompts, k) * SPLIT + c) * share, share)]

    def weight_copy(r, owner, c):
        place = weight_place(owner, 0, c)
        return pltpu.make_async_remote_copy(
            place, place, w_s.at[r, c], w_r.at[r, c], device_id={"head": lax.rem(head + r, heads)}
        )

    def spread_copy(r, k, c, sending):
        low = low_bit(k)
        place = weight_place(source(r), k - low if sending else k, c)
        return pltpu.make_async_remote_copy(
            place, place, v_s.at[r, k, c], v_r.at[r, k, c], device_id={"prompt": flipped(prompt, prompts, low)}
        )

    loads[0].wait()
    for h in range(SPLIT):
        for bit in lower_bits(n):
            query_copy(bit, h, bit).start()
    loads[5].wait()
    for c in range(SPLIT):
        for r in range(1, heads):
            weight_copy(r, head, c).start()

    def relay_queries(h):
        for r in relay_order(n):
            query_copy(r, h, low_bit(r)).wait_recv()
            for bit in lower_bits(low_bit(r)):
                query_copy(r + bit, h, bit).start()

    def spread_first(c):
        for r in range(1, heads):
            weight_copy(r, source(r), c).wait_recv()
            for bit in lower_bits(prompts):
                spread_copy(r, bit, c, True).start()

    def spread_rest(c):
        for r in range(1, heads):
            for k in relay_order(prompts):
                spread_copy(r, k, c, False).wait_recv()
                for bit in lower_bits(low_bit(k)):
                    spread_copy(r, k + bit, c, True).start()

    def spread_end(c):
        for r in range(1, heads):
            for k in range(1, prompts, 2):
                spread_copy(r, k, c, False).wait_recv()

    def prefix_part(asking, sample):
        keys = jnp.concatenate([pk[chosen[sample, j]] for j in range(MOST)], axis=0)
        values = jnp.concatenate([pv[chosen[sample, j]] for j in range(MOST)], axis=0)
        column = lax.broadcasted_iota(jnp.int32, (1, CHUNK), 1)
        hidden = jnp.where(column < chosen[sample, MOST] * BLOCK, 0.0, hidden_value)
        return softmax_part(scores_of(asking, keys) + hidden, values)

    asking = rows_of(qbuf[0])
    rows = asking.shape[0]
    last_seen = lengths[0] - tokens + lax.broadcasted_iota(jnp.int32, (rows, 1), 0) % tokens
    loads[1].wait()
    loads[2].wait()

    def own_scores(keys, start):
        column = start + lax.broadcasted_iota(jnp.int32, (1, keys.shape[0]), 1)
        return jnp.where(column <= last_seen, scores_of(asking, keys), hidden_value)

    def merged(one, two):
        maximum = jnp.maximum(one[0], two[0])
        shrink_one = jnp.exp2((one[0] - maximum) * factor)
        shrink_two = jnp.exp2((two[0] - maximum) * factor)
        return (
            maximum,
            one[1] * shrink_one + two[1] * shrink_two,
            one[2] * shrink_one + two[2] * shrink_two,
        )

    state = None
    for start in range(0, sk.shape[0], CHUNK):
        part = pl.ds(start, min(CHUNK, sk.shape[0] - start))
        latest = softmax_part(own_scores(sk[part], start), sv[part])
        state = latest if state is None else merged(state, latest)
    loads[3].wait()
    loads[4].wait()
    state = merged(state, prefix_part(asking, me))
    own_max[...] = jnp.broadcast_to(state[0], own_max.shape)
    own_sum[...] = jnp.broadcast_to(state[1], own_sum.shape)
    own_acc[...] = state[2]

    lane = lax.broadcasted_iota(jnp.int32, (piece, HD), 1)

    def remote_part(r, h):
        maximum, weight_sum, summed = prefix_part(rows_of(qbuf[r, span(h)]), partner(r))
        mean = (summed / jnp.maximum(weight_sum, 1e-30)).astype(jnp.bfloat16)
        top = jnp.zeros((piece, HD), jnp.float32)
        bottom = jnp.zeros((piece, HD), jnp.float32)
        for j in range(GQA):
            part = slice(j * piece, (j + 1) * piece)
            psend[r, span(h), j * HD : (j + 1) * HD] = mean[part]
            top = jnp.where(lane == j, maximum[part], top)
            bottom = jnp.where(lane == j, weight_sum[part], bottom)
        part_copy(r, h).start()
        square = jnp.concatenate([top, bottom, jnp.zeros((HD - 2 * piece, HD), jnp.float32)], axis=0)
        ssend[r, h] = square.T[: ssend.shape[2]]
        stat_copy(r, h).start()

    def odd_part(r, h):
        query_copy(r, h, 1).wait_recv()
        remote_part(r, h)

    relay_queries(0)
    for h in range(SPLIT):

        def even_step(i, carry):
            remote_part(2 * i + 2, h)
            return carry

        def odd_step(i, carry):
            odd_part(2 * i + 3, h)
            return carry

        lax.fori_loop(0, n // 2 - 1, even_step, 0)
        odd_part(1, h)
        if h + 1 < SPLIT:
            relay_queries(h + 1)
        lax.fori_loop(0, n // 2 - 1, odd_step, 0)
        spread_first(h)

    def stats_from(r, h):
        part_copy(r, h).wait_recv()
        stat_copy(r, h).wait_recv()
        padded = jnp.concatenate([sbuf[r, h], jnp.zeros((HD - sbuf.shape[2], HD), jnp.float32)], axis=0).T
        return padded[:piece], padded[piece : 2 * piece]

    def finish(r, h):
        reader, place = place_of(r)
        final_copy(r, h, 1).start()

        @pl.when(reader != head)
        def _():
            final_copy(r, h, 0).start()

        @pl.when(reader == head)
        def _():
            fbuf[head, place, span(h)] = att[r, span(h)]

    def merge_parts(h):
        stats = [stats_from(r, h) for r in range(1, n)]
        for j in range(GQA):
            part = pl.ds(j * tokens + h * piece, piece)
            columns = slice(j * HD, (j + 1) * HD)
            maximum = own_max[part]
            for top, _ in stats:
                maximum = jnp.maximum(maximum, top[:, j : j + 1])
            scale = jnp.exp2((own_max[part] - maximum) * factor)
            total = own_acc[part] * scale
            weight_sum = own_sum[part] * scale
            for r, (top, bottom) in zip(range(1, n), stats):
                portion = jnp.exp2((top[:, j : j + 1] - maximum) * factor) * bottom[:, j : j + 1]
                total = total + portion * pbuf[r, span(h), columns].astype(jnp.float32)
                weight_sum = weight_sum + portion
            att[0, span(h), columns] = (total / weight_sum).astype(jnp.bfloat16)
        for bit in lower_bits(n):
            if bit > 1:
                attended_copy(bit, h).start()
        finish(0, h)

    def relay_attended(h):
        for r in relay_order(n):
            attended_copy(r, h).wait_recv()
            for bit in lower_bits(low_bit(r)):
                if bit > 1:
                    attended_copy(r + bit, h).start()
            finish(r, h)

    def is_local(g, place):
        return (g == head) & ((head * per_head + place) % 2 == me % 2)

    def project(h):
        total = None
        for g in range(heads):
            for place in range(per_head):

                @pl.when(jnp.logical_not(is_local(g, place)))
                def _():
                    arrival(g, place, h).wait_recv()

        for g in range(heads):
            block = fbuf[g, :, span(h)].reshape(per_head * piece, fbuf.shape[-1])
            term = jnp.dot(block, wall[g], preferred_element_type=jnp.float32)
            total = term if total is None else total + term
        for place in range(per_head):
            out[pl.ds(place * tokens + h * piece, piece)] = total[place * piece : (place + 1) * piece]

    for h in range(SPLIT):
        merge_parts(h)
        spread_rest(h)
    for h in range(SPLIT):
        relay_attended(h)
    for c in range(SPLIT):
        spread_end(c)
    for h in range(SPLIT):
        project(h)

    for h in range(SPLIT):
        for r in range(1, n):
            query_copy(r, h, low_bit(r)).wait_send()
            part_copy(r, h).wait_send()
            stat_copy(r, h).wait_send()
        for r in range(0, n, 2):
            if r:
                attended_copy(r, h).wait_send()
            final_copy(r, h, 1).wait_send()

            @pl.when(place_of(r)[0] != head)
            def _():
                final_copy(r, h, 0).wait_send()

        for r in range(1, heads):
            weight_copy(r, head, h).wait_send()
            for k in range(1, prompts):
                spread_copy(r, k, h, True).wait_send()


def body(n, heads, prompts, queries, prefix_keys, prefix_values, suffix_keys, suffix_values, kept_blocks, suffix_lengths, out_weight):
    tokens, width = queries.shape[1:]
    blocks_here = prefix_keys.shape[0] // BLOCK
    slots = suffix_keys.shape[1]
    columns = out_weight.shape[1]
    per_head = n // heads
    assert prefix_keys.shape[1] == HD and width == GQA * HD and n % heads == 0
    assert n & (n - 1) == 0 and prompts & (prompts - 1) == 0 and per_head % 2 == 0
    bf16, f32 = jnp.bfloat16, jnp.float32
    any_space = pl.BlockSpec(memory_space=pltpu.HBM)
    smem = pl.BlockSpec(memory_space=pltpu.SMEM)
    dma = pltpu.SemaphoreType.DMA
    return pl.pallas_call(
        functools.partial(kernel, n, heads, prompts),
        out_shape=pltpu.VMEM((per_head * tokens, columns), f32),
        in_specs=[any_space] * 5 + [smem] * 2 + [any_space],
        out_specs=pl.BlockSpec(memory_space=pltpu.VMEM),
        scratch_shapes=[
            pltpu.VMEM((n, tokens, width), bf16),
            pltpu.VMEM((blocks_here, BLOCK, HD), bf16),
            pltpu.VMEM((blocks_here, BLOCK, HD), bf16),
            pltpu.VMEM((slots, HD), bf16),
            pltpu.VMEM((slots, HD), bf16),
            pltpu.VMEM((heads,) + out_weight.shape, bf16),
            pltpu.VMEM((GQA * tokens, HD), f32),
            pltpu.VMEM((GQA * tokens, HD), f32),
            pltpu.VMEM((GQA * tokens, HD), f32),
            pltpu.VMEM((n, tokens, width), bf16),
            pltpu.VMEM((n, tokens, width), bf16),
            pltpu.VMEM((n, SPLIT, 8, HD), f32),
            pltpu.VMEM((n, SPLIT, 8, HD), f32),
            pltpu.VMEM((n, tokens, width), bf16),
            pltpu.VMEM((heads, per_head, tokens, width), bf16),
            pltpu.SMEM((n, MOST + 1), jnp.int32),
            dma((6,)),
            dma((n, SPLIT)), dma((n, SPLIT)),
            dma((n, SPLIT)), dma((n, SPLIT)),
            dma((n, SPLIT)), dma((n, SPLIT)),
            dma((n, SPLIT)), dma((n, SPLIT)),
            dma((n // 2, 2, SPLIT)), dma((heads, per_head, SPLIT)),
            dma((heads, SPLIT)), dma((heads, SPLIT)),
            dma((heads, prompts, SPLIT)), dma((heads, prompts, SPLIT)),
        ],
        compiler_params=pltpu.CompilerParams(
            collective_id=0, has_side_effects=True, vmem_limit_bytes=63 * 1024 * 1024
        ),
    )(
        queries[0],
        prefix_keys.reshape(blocks_here, BLOCK, HD),
        prefix_values.reshape(blocks_here, BLOCK, HD),
        suffix_keys[0],
        suffix_values[0],
        kept_blocks,
        suffix_lengths,
        out_weight,
    )


def solution(mesh):
    in_specs = (
        P(("prompt", "seq"), None, "head"),
        P(("prompt", "seq"), "head"),
        P(("prompt", "seq"), "head"),
        P(("prompt", "seq"), None, "head"),
        P(("prompt", "seq"), None, "head"),
        P("prompt", None),
        P(("prompt", "seq")),
        P("head", "seq"),
    )
    out_specs = P(("prompt", "head"), "seq")
    part = functools.partial(body, mesh.shape["seq"], mesh.shape["head"], mesh.shape["prompt"])
    return jax.shard_map(part, mesh=mesh, in_specs=in_specs, out_specs=out_specs, check_vma=False)
```
